256 devices in a mesh: dp: 32 (over x, z), frames: 8 (over y, core).
Axes of the slice: x: 4, y: 4, z: 8, core: 2. Of those that a mesh axis runs over, the one named last changes fastest.
Arguments:
- token_ids: int32 [128], P('dp'), may hold values from 0 to 26623
- positions: int32 [128], P('dp'), may hold values from 1 to 255
- embed: bfloat16 [26624, 1280], P(('dp', 'frames')), may hold values from -32 to 32
- pos_table: bfloat16 [256, 1280], replicated, may hold values from -4 to 4
- self_keys: bfloat16 [128, 256, 1280], P('dp', 'frames'), may hold values from -150 to 150
- self_values: bfloat16 [128, 256, 1280], P('dp', 'frames'), may hold values from -6 to 6
- cross_keys: bfloat16 [128, 512, 1280], P('dp', 'frames'), may hold values from -150 to 150
- cross_values: bfloat16 [128, 512, 1280], P('dp', 'frames'), may hold values from -6 to 6
- norm_gains: float32 [4, 1280], replicated, may hold values from 0.1 to 1.9
- qkv_weight: bfloat16 [3, 1280, 1280], P(None, None, 'frames'), may hold values from -0.15625 to 0.15625
- out_weight: bfloat16 [1280, 1280], P(None, 'frames'), may hold values from -0.15625 to 0.15625
- cross_query_weight: bfloat16 [1280, 1280], P(None, 'frames'), may hold values from -0.15625 to 0.15625
- cross_out_weight: bfloat16 [1280, 1280], P(None, 'frames'), may hold values from -0.15625 to 0.15625
- up_weight: bfloat16 [1280, 5120], P(None, 'frames'), may hold values from -0.15625 to 0.15625
- down_weight: bfloat16 [5120, 1280], P('frames'), may hold values from -0.078125 to 0.078125
Outputs:
- log_probs: float32 [128, 26624], P(None, ('dp', 'frames'))
The draws below stay inside these ranges and needn't reach their ends.
Inputs may be any that keep to these rules, and one draw needn't show every extreme that they name: Stream s holds earlier tokens in cache slots 0 to positions[s] - 1; later slots are unused.
All inputs are finite; a program needn't handle non-finite values.
Results may differ from the reference program's by a relative error of at most 0.014.
Values may be sent and summed in bfloat16 or wider, within the bound.
A program may use at most 64 MiB of HBM per device.

```python
import math
import jax
import jax.numpy as jnp
import numpy as np
from jax import lax

D = 1280
HEADS = 20
HEAD_DIM = 64
FFN = 5120
VOCAB = 26624
STREAMS = 128
CACHE = 256
FRAMES = 512


def draw_embed(key, part):
    first, second = jax.random.split(jax.random.fold_in(key, 11), 2)
    base = jnp.clip(jax.random.normal(first, (VOCAB, D), jnp.float32), -6.0, 6.0)
    rise = 0.08 * 3.0 ** (jnp.arange(VOCAB, dtype=jnp.float32) / VOCAB)
    scale = rise * jax.random.uniform(second, (VOCAB,), jnp.float32, 0.8, 1.25)
    return (base * scale[:, None]).astype(jnp.bfloat16)


def draw_self_keys(key, part):
    first = jax.random.fold_in(jax.random.fold_in(key, 37), 0)
    base = jnp.clip(jax.random.normal(first, (STREAMS, CACHE, D), jnp.float32), -6.0, 6.0)
    return base.astype(jnp.bfloat16)


def draw_cross_keys(key, part):
    first = jax.random.fold_in(jax.random.fold_in(key, 23), 0)
    base = jnp.clip(jax.random.normal(first, (STREAMS, FRAMES, D), jnp.float32), -6.0, 6.0)
    return base.astype(jnp.bfloat16)


def plant(drawn, stream_key, smallest, largest):
    extent = drawn.shape
    index_at = [jax.random.randint(jax.random.fold_in(stream_key, axis), (), 0, extent[axis]) for axis in range(len(extent))]
    drawn = drawn.at[tuple(index_at)].set(smallest)
    longest = extent.index(max(extent))
    index_at[longest] = (index_at[longest] + 1) % extent[longest]
    return drawn.at[tuple(index_at)].set(largest)


def level_of(own_key, extent, cuts, low, largest):
    loudness, own = 1.0, jax.random.fold_in(own_key, 6)
    for position, parts in cuts:
        draws = jnp.exp(jax.random.uniform(jax.random.fold_in(own, position), (parts,), jnp.float32, low / len(cuts), largest / len(cuts)))
        loudness = loudness * jnp.repeat(draws, extent[position] // parts).reshape([-1 if axis == position else 1 for axis in range(len(extent))])
    return loudness


def rank_bounds(number_of, lean):
    loads = [(1 << 20) // math.isqrt(grade ** lean) + 1 for grade in range(1, number_of + 1)]
    width = 1 + sum(loads) // (1 << 30)
    return np.cumsum(np.array([max(1, weight // width) for weight in loads]))


def ranked_ids(key, shape, count, skew):
    table = rank_bounds(count, skew)
    pick = jax.random.randint(jax.random.fold_in(key, 1), shape, 0, int(table[count - 1]))
    grade = jnp.searchsorted(jnp.asarray(table, jnp.int32), pick, side="right")
    return jax.random.permutation(jax.random.fold_in(key, 2), count)[grade].astype(jnp.int32)


def noise(key, shape, deviation, reach, cuts=(), held_as=jnp.bfloat16):
    entries = jax.random.normal(key, shape, jnp.float32) * deviation
    if len(cuts) > 0:
        entries = level_of(key, shape, cuts, -0.22, 0.18) * entries
    return jnp.clip(entries, min=-reach, max=reach).astype(held_as)


def setup_inputs(seed: int = 0) -> dict:
    streams_of = jax.random.split(jax.random.key(seed), 16)
    token_ids = plant(ranked_ids(streams_of[0], (STREAMS,), VOCAB, 2), jax.random.fold_in(streams_of[0], 3), 0, VOCAB - 1).astype(jnp.int32)
    positions = plant(jax.random.randint(streams_of[1], (STREAMS,), 1, CACHE), jax.random.fold_in(streams_of[1], 1), 1, CACHE - 1).astype(jnp.int32)
    embed = draw_embed(jax.random.fold_in(streams_of[15], 71), 0)
    pos_table = noise(streams_of[3], (CACHE, D), 0.3, 4.0)
    self_keys = draw_self_keys(jax.random.fold_in(streams_of[15], 71), 0)
    self_values = noise(streams_of[5], (STREAMS, CACHE, D), 1.0, 6.0, ((0, 32), (1, 8)))
    cross_keys = draw_cross_keys(jax.random.fold_in(streams_of[15], 71), 0)
    cross_values = noise(streams_of[7], (STREAMS, FRAMES, D), 1.0, 6.0, ((0, 32), (1, 8)))
    norm_gains = jnp.clip(1.0 + 0.18 * jax.random.normal(streams_of[8], (4, D), jnp.float32), 0.1, 1.9)
    qkv_weight = noise(streams_of[9], (3, D, D), D ** -0.5, 0.15625, ((2, 8),))
    out_weight = noise(streams_of[10], (D, D), D ** -0.5, 0.15625, ((1, 8),))
    cross_query_weight = noise(streams_of[11], (D, D), D ** -0.5, 0.15625, ((1, 8),))
    cross_out_weight = noise(streams_of[12], (D, D), D ** -0.5, 0.15625, ((1, 8),))
    up_weight = noise(streams_of[13], (D, FFN), D ** -0.5, 0.15625, ((1, 8),))
    down_weight = noise(streams_of[14], (FFN, D), FFN ** -0.5, 0.078125, ((0, 8),))
    return dict(token_ids=token_ids, positions=positions, embed=embed, pos_table=pos_table, self_keys=self_keys, self_values=self_values, cross_keys=cross_keys, cross_values=cross_values, norm_gains=norm_gains, qkv_weight=qkv_weight, out_weight=out_weight, cross_query_weight=cross_query_weight, cross_out_weight=cross_out_weight, up_weight=up_weight, down_weight=down_weight)


def layer_norm(values, gain):
    mean = lax.optimization_barrier(jnp.mean(values, axis=-1, keepdims=True))
    centred = values - mean
    spread = lax.optimization_barrier(jnp.mean(centred * centred, axis=-1, keepdims=True))
    return centred / jnp.sqrt(spread + 1e-05) * gain

def heads_of(values):
    return values.reshape(values.shape[0], HEADS, HEAD_DIM).astype(jnp.float32)

def rounded(values):
    return lax.optimization_barrier(values.astype(jnp.bfloat16)).astype(jnp.float32)

def reference(token_ids, positions, embed, pos_table, self_keys, self_values, cross_keys, cross_values, norm_gains, qkv_weight, out_weight, cross_query_weight, cross_out_weight, up_weight, down_weight):
    streams = token_ids.shape[0]
    factor = jnp.float32(HEAD_DIM) ** (-0.5)
    start = embed[token_ids].astype(jnp.float32) + pos_table[positions].astype(jnp.float32)
    normed = layer_norm(start, norm_gains[0]).astype(jnp.bfloat16)
    qkv = jnp.einsum('sd,jde->jse', normed.astype(jnp.float32), qkv_weight.astype(jnp.float32)).astype(jnp.bfloat16)
    query, key_new, value_new = (heads_of(qkv[0]), heads_of(qkv[1]), heads_of(qkv[2]))
    keys4 = self_keys.astype(jnp.float32).reshape(streams, CACHE, HEADS, HEAD_DIM)
    vals4 = self_values.astype(jnp.float32).reshape(streams, CACHE, HEADS, HEAD_DIM)
    scores = jnp.einsum('she,sche->shc', query, keys4) * factor
    valid = jnp.arange(CACHE, dtype=jnp.int32)[None, :] < positions[:, None]
    scores = jnp.where(valid[:, None, :], scores, -jnp.inf)
    own = lax.optimization_barrier(jnp.sum(query * key_new, axis=-1)) * factor
    peak = jnp.maximum(lax.optimization_barrier(jnp.max(scores, axis=-1)), own)
    weights = jnp.exp(scores - peak[..., None])
    own_weight = jnp.exp(own - peak)
    total = lax.optimization_barrier(jnp.sum(weights, axis=-1)) + own_weight
    mixed = jnp.einsum('shc,sche->she', rounded(weights), vals4) + own_weight[..., None] * value_new
    self_mix = (mixed / total[..., None]).reshape(streams, D).astype(jnp.bfloat16)
    self_out = jnp.dot(self_mix, out_weight, preferred_element_type=jnp.float32).astype(jnp.bfloat16)
    after_self = start + self_out.astype(jnp.float32)
    normed2 = layer_norm(after_self, norm_gains[1]).astype(jnp.bfloat16)
    cross_query = heads_of(jnp.dot(normed2, cross_query_weight, preferred_element_type=jnp.float32).astype(jnp.bfloat16))
    ckeys = cross_keys.astype(jnp.float32).reshape(streams, FRAMES, HEADS, HEAD_DIM)
    cvals = cross_values.astype(jnp.float32).reshape(streams, FRAMES, HEADS, HEAD_DIM)
    cscores = jnp.einsum('she,sfhe->shf', cross_query, ckeys) * factor
    ctop = lax.optimization_barrier(jnp.max(cscores, axis=-1))
    cweights = jnp.exp(cscores - ctop[..., None])
    ctotal = lax.optimization_barrier(jnp.sum(cweights, axis=-1))
    cmixed = jnp.einsum('shf,sfhe->she', rounded(cweights), cvals) / ctotal[..., None]
    cross_mix = cmixed.reshape(streams, D).astype(jnp.bfloat16)
    cross_out = jnp.dot(cross_mix, cross_out_weight, preferred_element_type=jnp.float32).astype(jnp.bfloat16)
    after_cross = after_self + cross_out.astype(jnp.float32)
    normed3 = layer_norm(after_cross, norm_gains[2]).astype(jnp.bfloat16)
    hidden = jax.nn.gelu(jnp.dot(normed3, up_weight, preferred_element_type=jnp.float32), approximate=False).astype(jnp.bfloat16)
    after_mlp = after_cross + jnp.dot(hidden, down_weight, preferred_element_type=jnp.float32)
    final = layer_norm(after_mlp, norm_gains[3]).astype(jnp.bfloat16)
    logits = jnp.dot(final, embed.T, preferred_element_type=jnp.float32)
    top = lax.optimization_barrier(jnp.max(logits, axis=-1, keepdims=True))
    return logits - top - jnp.log(lax.optimization_barrier(jnp.sum(jnp.exp(logits - top), axis=-1, keepdims=True)))
```

```python
import functools

import jax
import jax.numpy as jnp
from jax import lax
from jax.experimental import pallas as pl
from jax.experimental.pallas import tpu as pltpu
from jax.sharding import PartitionSpec as P

MESH = pl.DeviceIdType.MESH
F32, BF16, I32 = jnp.float32, jnp.bfloat16, jnp.int32
HEADS = 20
WIDTH = 1280
TILES = WIDTH // 128
NF = 8
PIECE = WIDTH // NF
NEG = -1e30
FIRST_TILE = [PIECE * k // 128 for k in range(NF)]


def nt(a, b):
    return lax.dot_general(a, b, (((1,), (1,)), ((), ())), preferred_element_type=F32)


def nn(a, b):
    return jnp.dot(a, b, preferred_element_type=F32)


def kernel(nd, vocab, slots, frames, hidden,
           tok_ref, pos_ref, emb_h, post_h, sk_h, sv_h, ck_h, cv_h, gain_h, qkv_h, ow_h, cqw_h, cow_h, up_h, down_h,
           out_ref,
           emb, post, sk, sv, ck, cv, gain, qkvw, ow, cqw, cow, up, down,
           pqkv, pow_, pcq, pco,
           ids_buf, ew, row_send, row_buf, tok_buf, qkv_buf, smix, sstat, so_buf, cq_buf, cmix, cstat, co_buf, dn_buf,
           fin_buf, st1, st2,
           lsem, ssem, rsem):
    d = lax.axis_index("dp")
    f = lax.axis_index("frames")
    sub = lax.broadcasted_iota(I32, (8, 128), 0)
    lane = lax.broadcasted_iota(I32, (8, 128), 1)
    low = sub < 4
    own_half = (sub // 4) == (lane // 64)

    def roll4(v):
        return pltpu.roll(v, 4, v.ndim - 2)

    pairs = [(emb_h, emb), (post_h, post), (qkv_h, qkvw), (gain_h, gain), (sk_h, sk), (sv_h, sv), (ow_h, ow),
             (cqw_h, cqw), (ck_h, ck), (cv_h, cv), (cow_h, cow), (up_h, up), (down_h, down)]
    local = {}
    for n, (src, dst) in enumerate(pairs):
        local[n] = pltpu.make_async_copy(src, dst, lsem.at[n])
        local[n].start()
    EMB, POST, QKV, GAIN, SK, SV, OW, CQW, CK, CV, COW, UP, DOWN = range(13)

    barrier = pltpu.get_barrier_semaphore()
    for k in range(1, nd):
        pl.semaphore_signal(barrier, inc=1, device_id=(lax.rem(d + k, nd), f), device_id_type=MESH)
    for k in range(1, NF):
        pl.semaphore_signal(barrier, inc=1, device_id=(d, lax.rem(f + k, NF)), device_id_type=MESH)

    exchanges = []

    def frames_send(n, buf):
        for k in range(1, NF):
            pltpu.make_async_remote_copy(
                src_ref=buf.at[f], dst_ref=buf.at[f], send_sem=ssem.at[n], recv_sem=rsem.at[n],
                device_id=(d, lax.rem(f + k, NF)), device_id_type=MESH).start()
        exchanges.append((n, buf, NF - 1))

    def dp_send(n, buf):
        for k in range(1, nd):
            pltpu.make_async_remote_copy(
                src_ref=buf.at[d], dst_ref=buf.at[d], send_sem=ssem.at[n], recv_sem=rsem.at[n],
                device_id=(lax.rem(d + k, nd), f), device_id_type=MESH).start()
        exchanges.append((n, buf, nd - 1))

    def received(n, buf, count):
        pltpu.make_async_copy(buf.at[pl.ds(0, count)], buf.at[pl.ds(0, count)], rsem.at[n]).wait()

    t0, t1, t2, t3 = (tok_ref[s] for s in range(4))
    p0, p1, p2, p3 = (pos_ref[s] for s in range(4))

    def by_stream(index, a, b, c, e):
        return jnp.where(index == 0, a, jnp.where(index == 1, b, jnp.where(index == 2, c, e)))

    ids_buf[d] = by_stream(sub % 4, t0, t1, t2, t3)
    pl.semaphore_wait(barrier, nd - 1 + NF - 1)
    dp_send(0, ids_buf)

    def first_lane(index):
        return pl.multiple_of(lax.div(index * 5, 4) * 128, 128)

    local[EMB].wait()
    for k in range(1, NF):
        peer = lax.rem(f + k, NF)
        pltpu.make_async_remote_copy(
            src_ref=emb.at[:, pl.ds(first_lane(peer), 256)], dst_ref=ew.at[f], send_sem=ssem.at[1], recv_sem=rsem.at[1],
            device_id=(d, peer), device_id_type=MESH).start()
    exchanges.append((1, ew, NF - 1))
    ew[f] = emb[:, pl.ds(first_lane(f), 256)]

    local[POST].wait()
    places = post.shape[0]
    place_at = by_stream(lax.broadcasted_iota(I32, (8, places), 0) % 4, p0, p1, p2, p3)
    place_hit = (lax.broadcasted_iota(I32, (8, places), 1) == place_at).astype(F32).astype(BF16)
    place = nn(place_hit, post[...])

    shift = lax.rem(f, 4) * 32
    move = (lax.broadcasted_iota(I32, (PIECE, 256), 1)
            == lax.broadcasted_iota(I32, (PIECE, 256), 0) + shift).astype(F32).astype(BF16)
    local[QKV].wait()
    for j in range(3):
        pqkv[j] = nn(qkvw[j], move).astype(BF16)
    local[OW].wait()
    pow_[...] = nn(ow[...], move).astype(BF16)
    local[CQW].wait()
    pcq[...] = nn(cqw[...], move).astype(BF16)
    local[COW].wait()
    pco[...] = nn(cow[...], move).astype(BF16)

    received(1, ew, NF - 1)
    received(0, ids_buf, nd - 1)
    ids = ids_buf[...].reshape(nd * 8, 128)[:, :vocab]
    row_of = lax.broadcasted_iota(I32, (nd * 8, vocab), 1)
    found = None
    for j in range(NF):
        hit = (ids == row_of + (d * NF + j) * vocab).astype(F32).astype(BF16)
        part = nn(hit, ew[j])
        found = part if found is None else found + part
    low_rows = (lax.broadcasted_iota(I32, (nd * 8, 128), 0) % 8) < 4
    folded = jnp.where(low_rows, found[:, :128], found[:, 128:])
    row_send[...] = folded.reshape(nd, 8, 128).astype(BF16)
    for k in range(1, nd):
        peer = lax.rem(d + k, nd)
        pltpu.make_async_remote_copy(
            src_ref=row_send.at[peer], dst_ref=row_buf.at[d], send_sem=ssem.at[2], recv_sem=rsem.at[2],
            device_id=(peer, f), device_id_type=MESH).start()
    exchanges.append((2, row_buf, nd - 1))
    row_buf[d] = row_send[d]
    received(2, row_buf, nd - 1)
    tok_buf[f] = jnp.sum(row_buf[...].astype(F32), axis=0).astype(BF16)
    frames_send(3, tok_buf)
    local[GAIN].wait()
    received(3, tok_buf, NF - 1)

    def unfold(v):
        other = roll4(v)
        return jnp.where(low, v, other), jnp.where(low, other, v)

    tiles = [None] * TILES
    for k in range(NF):
        first, second = unfold(tok_buf[k].astype(F32))
        tiles[FIRST_TILE[k]] = first
        if tiles[FIRST_TILE[k] + 1] is None:
            tiles[FIRST_TILE[k] + 1] = second
    start = jnp.concatenate(tiles, axis=1) + place

    def norm(values, row):
        mean = jnp.sum(values, axis=1, keepdims=True) * (1.0 / WIDTH)
        centred = values - mean
        spread = jnp.sum(centred * centred, axis=1, keepdims=True) * (1.0 / WIDTH)
        return (centred * lax.rsqrt(spread + 1e-5) * gain[row : row + 1, :]).astype(BF16)

    def fold_window(v):
        return jnp.where(low, v[:, :128], v[:, 128:]).astype(BF16)

    def columns_joined(pieces):
        tiles = [None] * TILES
        for k in range(NF):
            for at, part in zip((FIRST_TILE[k], FIRST_TILE[k] + 1), unfold(pieces[k].astype(F32))):
                tiles[at] = part if tiles[at] is None else tiles[at] + part
        return tiles

    normed = norm(start, 0)
    qkv_buf[f] = jnp.stack([fold_window(nn(normed, pqkv[j])) for j in range(3)])
    frames_send(4, qkv_buf)

    rows_r = 4 * HEADS

    def attend(query, key_ref, value_ref, count, valid, own):
        zero = jnp.zeros((8, 128), F32)
        blocks = []
        for t in range(TILES):
            block = [zero] * TILES
            block[t] = jnp.where(own_half, query[t], 0.0)
            blocks.append(jnp.concatenate(block, axis=1))
        spread_query = jnp.concatenate(blocks, axis=0).astype(BF16)
        keys = key_ref[...].reshape(4 * count, WIDTH)
        values = value_ref[...].reshape(4 * count, WIDTH)
        scores = nt(spread_query, keys) * 0.125
        scores = jnp.where(valid, scores, NEG)
        peak = jnp.max(scores, axis=1, keepdims=True)
        if own is not None:
            own_score = jnp.concatenate(own[0], axis=0)
            peak = jnp.maximum(peak, own_score)
        weights = jnp.where(valid, jnp.exp(scores - peak), 0.0)
        total = jnp.sum(weights, axis=1, keepdims=True)
        if own is not None:
            own_weight = jnp.where(own_score > 0.5 * NEG, jnp.exp(own_score - peak), 0.0)
            total = total + own_weight
        some = total > 0.0
        inverse = jnp.where(some, 1.0 / jnp.where(some, total, 1.0), 0.0)
        level = jnp.where(some, peak + jnp.log(jnp.where(some, total, 1.0)), NEG)
        stat = jnp.zeros((8, 128), F32)
        raw = []
        for t in range(TILES):
            at = slice(8 * t, 8 * t + 8)
            mixed = nn(weights[at].astype(BF16), values[:, 128 * t : 128 * t + 128])
            if own is not None:
                mixed = mixed + own_weight[at] * own[1][t]
            raw.append(mixed * inverse[at])
            stat = jnp.where(lane == t, level[at], stat)
        half = TILES // 2
        mix = [jnp.where(own_half, raw[t], roll4(raw[t + half])).astype(BF16) for t in range(half)]
        return jnp.stack(mix), stat

    def joined(mix_buf, stat_buf):
        levels = [stat_buf[k] for k in range(NF)]
        top = functools.reduce(jnp.maximum, levels)
        shares = [jnp.exp(v - top) for v in levels]
        inverse = 1.0 / functools.reduce(jnp.add, shares)
        shares = [v * inverse for v in shares]
        turned = [roll4(v) for v in shares]
        half = TILES // 2
        first, second = [], []
        for t in range(half):
            total = None
            for k in range(NF):
                share = jnp.where(own_half, jnp.broadcast_to(shares[k][:, t : t + 1], (8, 128)),
                                  jnp.broadcast_to(turned[k][:, t + half : t + half + 1], (8, 128)))
                term = share * mix_buf[k, t].astype(F32)
                total = term if total is None else total + term
            other = roll4(total)
            first.append(jnp.where(own_half, total, other))
            second.append(jnp.where(own_half, other, total))
        return jnp.concatenate(first + second, axis=1).astype(BF16)

    column = lax.broadcasted_iota(I32, (rows_r, 4 * slots), 1)
    same = (lax.broadcasted_iota(I32, (rows_r, 4 * slots), 0) % 4) == column // slots
    here = by_stream(column // slots, p0, p1, p2, p3)
    valid = jnp.logical_and(same, f * slots + column % slots < here)
    column = lax.broadcasted_iota(I32, (rows_r, 4 * frames), 1)
    every = (lax.broadcasted_iota(I32, (rows_r, 4 * frames), 0) % 4) == column // frames

    local[SK].wait()
    local[SV].wait()
    received(4, qkv_buf, NF - 1)
    query, key_new, value_new = (columns_joined([qkv_buf[k, j] for k in range(NF)]) for j in range(3))
    first_device = f == 0
    own_scores = []
    for t in range(TILES):
        score = jnp.sum(jnp.where(own_half, query[t] * key_new[t], 0.0), axis=1, keepdims=True) * 0.125
        own_scores.append(jnp.where(first_device, score, NEG))
    smix[f], sstat[f] = attend(query, sk, sv, slots, valid, (own_scores, value_new))
    frames_send(5, sstat)
    frames_send(6, smix)
    received(5, sstat, NF - 1)
    received(6, smix, NF - 1)
    self_mix = joined(smix, sstat)

    so_buf[f] = fold_window(nn(self_mix, pow_[...]))
    frames_send(7, so_buf)
    received(7, so_buf, NF - 1)
    after_self = start + jnp.concatenate(columns_joined([so_buf[k] for k in range(NF)]), axis=1)
    normed2 = norm(after_self, 1)
    cq_buf[f] = fold_window(nn(normed2, pcq[...]))
    frames_send(8, cq_buf)
    local[CK].wait()
    local[CV].wait()
    received(8, cq_buf, NF - 1)
    cross_query = columns_joined([cq_buf[k] for k in range(NF)])
    cmix[f], cstat[f] = attend(cross_query, ck, cv, frames, every, None)
    frames_send(9, cstat)
    frames_send(10, cmix)
    received(9, cstat, NF - 1)
    received(10, cmix, NF - 1)
    cross_mix = joined(cmix, cstat)
    co_buf[f] = fold_window(nn(cross_mix, pco[...]))
    frames_send(11, co_buf)
    local[UP].wait()
    local[DOWN].wait()
    received(11, co_buf, NF - 1)
    after_cross = after_self + jnp.concatenate(columns_joined([co_buf[k] for k in range(NF)]), axis=1)

    normed3 = norm(after_cross, 2)
    raised = nn(normed3, up[...])
    active = (raised * (1.0 + lax.erf(raised * (0.5 ** 0.5))) * 0.5).astype(BF16)
    lowered = nn(active, down[...])
    half = TILES // 2

    def tile(v, t):
        return v[:, 128 * t : 128 * t + 128]

    dn_buf[f] = jnp.stack([jnp.where(low, tile(lowered, t), tile(lowered, t + half)).astype(BF16) for t in range(half)])
    frames_send(12, dn_buf)
    received(12, dn_buf, NF - 1)
    summed = jnp.sum(dn_buf[...].astype(F32), axis=0)
    halves = [unfold(summed[t]) for t in range(half)]
    after_mlp = after_cross + jnp.concatenate([a for a, _ in halves] + [b for _, b in halves], axis=1)
    final = norm(after_mlp, 3).astype(F32)
    fin_buf[d] = jnp.stack([jnp.where(low, tile(final, t), tile(final, t + half)).astype(BF16) for t in range(half)])
    dp_send(13, fin_buf)
    received(13, fin_buf, nd - 1)

    low3 = lax.broadcasted_iota(I32, (nd // 2, 8, 128), 1) < 4
    first, second = [], []
    for t in range(half):
        both = fin_buf[:, t].astype(F32)
        turned = roll4(both).reshape(nd // 2, 2, 8, 128)
        both = both.reshape(nd // 2, 2, 8, 128)
        first.append(jnp.where(low3, both[:, 0], turned[:, 1]).reshape(nd * 4, 128))
        second.append(jnp.where(low3, turned[:, 0], both[:, 1]).reshape(nd * 4, 128))
    logits = nt(jnp.concatenate(first + second, axis=1).astype(BF16), emb[...])
    peak = jnp.max(logits, axis=1, keepdims=True)
    level = peak + jnp.log(jnp.sum(jnp.exp(logits - peak), axis=1, keepdims=True))
    st1[f] = jnp.transpose(jnp.broadcast_to(level, (nd * 4, 128)))[0:1]
    frames_send(14, st1)
    received(14, st1, NF - 1)

    def joined_levels(levels):
        top = jnp.max(levels, axis=0)
        return top + jnp.log(jnp.sum(jnp.exp(levels - top[None]), axis=0))

    st2[d] = joined_levels(st1[...])
    dp_send(15, st2)
    received(15, st2, nd - 1)
    whole = joined_levels(st2[...])
    out_ref[...] = logits - jnp.transpose(jnp.broadcast_to(whole, (128, nd * 4)))[:, :vocab]

    for n, buf, count in exchanges:
        pltpu.make_async_copy(buf.at[pl.ds(0, count)], buf.at[pl.ds(0, count)], ssem.at[n]).wait()


def on_device(nd, *args):
    (token_ids, positions, embed, pos_table, self_keys, self_values, cross_keys, cross_values, norm_gains, qkv_weight,
     out_weight, cross_query_weight, cross_out_weight, up_weight, down_weight) = args
    vocab = embed.shape[0]
    slots, frames, hidden = self_keys.shape[1], cross_keys.shape[1], up_weight.shape[1]
    streams = nd * 4
    vm = pltpu.VMEM
    big = args[2:]
    held = [vm(a.shape, a.dtype) for a in big]
    scratch = held + [
        vm((3, WIDTH, 256), BF16), vm((WIDTH, 256), BF16), vm((WIDTH, 256), BF16), vm((WIDTH, 256), BF16),
        vm((nd, 8, 128), I32),
        vm((NF, vocab, 256), BF16),
        vm((nd, 8, 128), BF16), vm((nd, 8, 128), BF16),
        vm((NF, 8, 128), BF16),
        vm((NF, 3, 8, 128), BF16),
        vm((NF, TILES // 2, 8, 128), BF16), vm((NF, 8, 128), F32),
        vm((NF, 8, 128), BF16), vm((NF, 8, 128), BF16),
        vm((NF, TILES // 2, 8, 128), BF16), vm((NF, 8, 128), F32),
        vm((NF, 8, 128), BF16),
        vm((NF, TILES // 2, 8, 128), BF16),
        vm((nd, TILES // 2, 8, 128), BF16),
        vm((NF, 1, streams), F32), vm((nd, 1, streams), F32),
        pltpu.SemaphoreType.DMA((len(big),)), pltpu.SemaphoreType.DMA((16,)), pltpu.SemaphoreType.DMA((16,)),
    ]
    return pl.pallas_call(
        functools.partial(kernel, nd, vocab, slots, frames, hidden),
        out_shape=jax.ShapeDtypeStruct((streams, vocab), F32),
        in_specs=[pl.BlockSpec(memory_space=pltpu.SMEM)] * 2 + [pl.BlockSpec(memory_space=pl.ANY)] * len(big),
        out_specs=pl.BlockSpec(memory_space=pltpu.VMEM),
        scratch_shapes=scratch,
        compiler_params=pltpu.CompilerParams(collective_id=0, has_side_effects=True, vmem_limit_bytes=60 * 1024 * 1024),
    )(*args)


def solution(mesh):
    nd = mesh.shape["dp"]
    both = ("dp", "frames")
    in_specs = (
        P("dp"), P("dp"), P(both, None), P(),
        P("dp", "frames", None), P("dp", "frames", None), P("dp", "frames", None), P("dp", "frames", None),
        P(), P(None, None, "frames"), P(None, "frames"), P(None, "frames"), P(None, "frames"), P(None, "frames"),
        P("frames", None),
    )
    return jax.shard_map(functools.partial(on_device, nd), mesh=mesh, in_specs=in_specs, out_specs=P(None, both),
                         check_vma=False)
```

```python
import functools

import jax
import jax.numpy as jnp
from jax import lax
from jax.experimental import pallas as pl
from jax.experimental.pallas import tpu as pltpu
from jax.sharding import PartitionSpec as P

MESH = pl.DeviceIdType.MESH
PHASES = False
F32, BF16, I32 = jnp.float32, jnp.bfloat16, jnp.int32
HEADS = 20
WIDTH = 1280
TILES = WIDTH // 128
NF = 8
PIECE = WIDTH // NF
NEG = -1e30
FIRST_TILE = [PIECE * k // 128 for k in range(NF)]


def nt(a, b):
    return lax.dot_general(a, b, (((1,), (1,)), ((), ())), preferred_element_type=F32)


def nn(a, b):
    return jnp.dot(a, b, preferred_element_type=F32)


def kernel(nd, vocab, slots, frames, hidden,
           tok_ref, pos_ref, emb_h, post_h, sk_h, sv_h, ck_h, cv_h, gain_h, qkv_h, ow_h, cqw_h, cow_h, up_h, down_h,
           out_ref,
           emb, post, sk, sv, ck, cv, gain, up, down,
           pqkv, pow_, pcq, pco,
           ids_buf, ew, row_send, row_buf, tok_buf, qkv_buf, smix, sstat, so_buf, cq_buf, cmix, cstat, co_buf, dn_buf,
           fin_buf, st1, st2,
           lsem, ssem, rsem):
    d = lax.axis_index("dp")
    f = lax.axis_index("frames")
    sub = lax.broadcasted_iota(I32, (8, 128), 0)
    lane = lax.broadcasted_iota(I32, (8, 128), 1)
    low = sub < 4
    own_half = (sub // 4) == (lane // 64)

    scopes = []

    def phase(name):
        if PHASES:
            if scopes:
                scopes.pop().__exit__(None, None, None)
            if name:
                scopes.append(jax.named_scope(name))
                scopes[0].__enter__()

    phase("load")

    def roll4(v):
        return pltpu.roll(v, 4, v.ndim - 2)

    window = pl.ds(pl.multiple_of(lax.rem(f, 4) * 32, 32), PIECE)
    pairs = [(emb_h, emb), (post_h, post), (qkv_h, pqkv.at[:, window, :]), (gain_h, gain), (sk_h, sk), (sv_h, sv),
             (ow_h, pow_.at[window, :]), (cqw_h, pcq.at[window, :]), (ck_h, ck), (cv_h, cv), (cow_h, pco.at[window, :]),
             (up_h, up), (down_h, down)]
    local = {}
    for n, (src, dst) in enumerate(pairs):
        local[n] = pltpu.make_async_copy(src, dst, lsem.at[n])
        local[n].start()
    EMB, POST, QKV, GAIN, SK, SV, OW, CQW, CK, CV, COW, UP, DOWN = range(13)

    barrier = pltpu.get_barrier_semaphore()
    for k in range(1, nd):
        pl.semaphore_signal(barrier, inc=1, device_id=(lax.rem(d + k, nd), f), device_id_type=MESH)
    for k in range(1, NF):
        pl.semaphore_signal(barrier, inc=1, device_id=(d, lax.rem(f + k, NF)), device_id_type=MESH)

    exchanges = []

    def frames_send(n, buf):
        for k in range(1, NF):
            pltpu.make_async_remote_copy(
                src_ref=buf.at[f], dst_ref=buf.at[f], send_sem=ssem.at[n], recv_sem=rsem.at[n],
                device_id=(d, lax.rem(f + k, NF)), device_id_type=MESH).start()
        exchanges.append((n, buf, NF - 1))

    def dp_send(n, buf):
        for k in range(1, nd):
            pltpu.make_async_remote_copy(
                src_ref=buf.at[d], dst_ref=buf.at[d], send_sem=ssem.at[n], recv_sem=rsem.at[n],
                device_id=(lax.rem(d + k, nd), f), device_id_type=MESH).start()
        exchanges.append((n, buf, nd - 1))

    def received(n, buf, count):
        pltpu.make_async_copy(buf.at[pl.ds(0, count)], buf.at[pl.ds(0, count)], rsem.at[n]).wait()

    t0, t1, t2, t3 = (tok_ref[s] for s in range(4))
    p0, p1, p2, p3 = (pos_ref[s] for s in range(4))

    def by_stream(index, a, b, c, e):
        return jnp.where(index == 0, a, jnp.where(index == 1, b, jnp.where(index == 2, c, e)))

    ids_buf[d] = by_stream(sub % 4, t0, t1, t2, t3)
    phase("barrier")
    pl.semaphore_wait(barrier, nd - 1 + NF - 1)
    phase("ids_send")
    dp_send(0, ids_buf)

    def first_lane(index):
        return pl.multiple_of(lax.div(index * 5, 4) * 128, 128)

    local[EMB].wait()
    for k in range(1, NF):
        peer = lax.rem(f + k, NF)
        pltpu.make_async_remote_copy(
            src_ref=emb.at[:, pl.ds(first_lane(peer), 256)], dst_ref=ew.at[f], send_sem=ssem.at[1], recv_sem=rsem.at[1],
            device_id=(d, peer), device_id_type=MESH).start()
    exchanges.append((1, ew, NF - 1))
    ew[f] = emb[:, pl.ds(first_lane(f), 256)]

    phase("idle_work")
    local[POST].wait()
    places = post.shape[0]
    place_at = by_stream(lax.broadcasted_iota(I32, (8, places), 0) % 4, p0, p1, p2, p3)
    place_hit = (lax.broadcasted_iota(I32, (8, places), 1) == place_at).astype(F32).astype(BF16)
    place = nn(place_hit, post[...])

    for i in range(3):
        rest = pl.ds(pl.multiple_of(lax.rem(lax.rem(f, 4) + 5 + i, 8) * 32, 32), 32)
        pqkv[:, rest, :] = jnp.zeros((3, 32, WIDTH), BF16)
        for ref in (pow_, pcq, pco):
            ref[rest, :] = jnp.zeros((32, WIDTH), BF16)

    phase("ids_wait")
    received(1, ew, NF - 1)
    received(0, ids_buf, nd - 1)
    phase("onehot")
    ids = ids_buf[...].reshape(nd * 8, 128)[:, :vocab]
    row_of = lax.broadcasted_iota(I32, (nd * 8, vocab), 1)
    found = None
    for j in range(NF):
        hit = (ids == row_of + (d * NF + j) * vocab).astype(F32).astype(BF16)
        part = nn(hit, ew[j])
        found = part if found is None else found + part
    low_rows = (lax.broadcasted_iota(I32, (nd * 8, 128), 0) % 8) < 4
    folded = jnp.where(low_rows, found[:, :128], found[:, 128:])
    row_send[...] = folded.reshape(nd, 8, 128).astype(BF16)
    phase("rows_send")
    for k in range(1, nd):
        peer = lax.rem(d + k, nd)
        pltpu.make_async_remote_copy(
            src_ref=row_send.at[peer], dst_ref=row_buf.at[d], send_sem=ssem.at[2], recv_sem=rsem.at[2],
            device_id=(peer, f), device_id_type=MESH).start()
    exchanges.append((2, row_buf, nd - 1))
    phase("rows_wait")
    row_buf[d] = row_send[d]
    received(2, row_buf, nd - 1)
    phase("rows_sum")
    tok_buf[f] = jnp.sum(row_buf[...].astype(F32), axis=0).astype(BF16)
    phase("tok_x")
    frames_send(3, tok_buf)
    local[GAIN].wait()
    received(3, tok_buf, NF - 1)

    phase("ln1")
    def unfold(v):
        other = roll4(v)
        return jnp.where(low, v, other), jnp.where(low, other, v)

    tiles = [None] * TILES
    for k in range(NF):
        first, second = unfold(tok_buf[k].astype(F32))
        tiles[FIRST_TILE[k]] = first
        if tiles[FIRST_TILE[k] + 1] is None:
            tiles[FIRST_TILE[k] + 1] = second
    start = jnp.concatenate(tiles, axis=1) + place

    def norm(values, row):
        mean = jnp.sum(values, axis=1, keepdims=True) * (1.0 / WIDTH)
        centred = values - mean
        spread = jnp.sum(centred * centred, axis=1, keepdims=True) * (1.0 / WIDTH)
        return (centred * lax.rsqrt(spread + 1e-5) * gain[row : row + 1, :]).astype(BF16)

    def fold_window(v):
        return jnp.where(low, v[:, :128], v[:, 128:]).astype(BF16)

    def columns_joined(pieces):
        tiles = [None] * TILES
        for k in range(NF):
            for at, part in zip((FIRST_TILE[k], FIRST_TILE[k] + 1), unfold(pieces[k].astype(F32))):
                tiles[at] = part if tiles[at] is None else tiles[at] + part
        return tiles

    normed = norm(start, 0)
    local[QKV].wait()
    phase("qkv_mm")
    qkv_buf[f] = jnp.stack([fold_window(nt(normed, pqkv[j])) for j in range(3)])
    phase("qkv_x")
    frames_send(4, qkv_buf)

    rows_r = 4 * HEADS

    def attend(query, key_ref, value_ref, count, valid, own):
        zero = jnp.zeros((8, 128), F32)
        blocks = []
        for t in range(TILES):
            block = [zero] * TILES
            block[t] = jnp.where(own_half, query[t], 0.0)
            blocks.append(jnp.concatenate(block, axis=1))
        spread_query = jnp.concatenate(blocks, axis=0).astype(BF16)
        keys = key_ref[...].reshape(4 * count, WIDTH)
        values = value_ref[...].reshape(4 * count, WIDTH)
        scores = nt(spread_query, keys) * 0.125
        scores = jnp.where(valid, scores, NEG)
        peak = jnp.max(scores, axis=1, keepdims=True)
        if own is not None:
            own_score = jnp.concatenate(own[0], axis=0)
            peak = jnp.maximum(peak, own_score)
        weights = jnp.where(valid, jnp.exp(scores - peak), 0.0)
        total = jnp.sum(weights, axis=1, keepdims=True)
        if own is not None:
            own_weight = jnp.where(own_score > 0.5 * NEG, jnp.exp(own_score - peak), 0.0)
            total = total + own_weight
        some = total > 0.0
        inverse = jnp.where(some, 1.0 / jnp.where(some, total, 1.0), 0.0)
        level = jnp.where(some, peak + jnp.log(jnp.where(some, total, 1.0)), NEG)
        stat = jnp.zeros((8, 128), F32)
        raw = []
        for t in range(TILES):
            at = slice(8 * t, 8 * t + 8)
            mixed = nn(weights[at].astype(BF16), values[:, 128 * t : 128 * t + 128])
            if own is not None:
                mixed = mixed + own_weight[at] * own[1][t]
            raw.append(mixed * inverse[at])
            stat = jnp.where(lane == t, level[at], stat)
        half = TILES // 2
        mix = [jnp.where(own_half, raw[t], roll4(raw[t + half])).astype(BF16) for t in range(half)]
        return jnp.stack(mix), stat

    def joined(mix_buf, stat_buf):
        levels = [stat_buf[k] for k in range(NF)]
        top = functools.reduce(jnp.maximum, levels)
        shares = [jnp.exp(v - top) for v in levels]
        inverse = 1.0 / functools.reduce(jnp.add, shares)
        shares = [v * inverse for v in shares]
        turned = [roll4(v) for v in shares]
        half = TILES // 2
        first, second = [], []
        for t in range(half):
            total = None
            for k in range(NF):
                share = jnp.where(own_half, jnp.broadcast_to(shares[k][:, t : t + 1], (8, 128)),
                                  jnp.broadcast_to(turned[k][:, t + half : t + half + 1], (8, 128)))
                term = share * mix_buf[k, t].astype(F32)
                total = term if total is None else total + term
            other = roll4(total)
            first.append(jnp.where(own_half, total, other))
            second.append(jnp.where(own_half, other, total))
        return jnp.concatenate(first + second, axis=1).astype(BF16)

    column = lax.broadcasted_iota(I32, (rows_r, 4 * slots), 1)
    same = (lax.broadcasted_iota(I32, (rows_r, 4 * slots), 0) % 4) == column // slots
    here = by_stream(column // slots, p0, p1, p2, p3)
    valid = jnp.logical_and(same, f * slots + column % slots < here)
    column = lax.broadcasted_iota(I32, (rows_r, 4 * frames), 1)
    every = (lax.broadcasted_iota(I32, (rows_r, 4 * frames), 0) % 4) == column // frames

    local[SK].wait()
    local[SV].wait()
    received(4, qkv_buf, NF - 1)
    phase("attn1")
    query, key_new, value_new = (columns_joined([qkv_buf[k, j] for k in range(NF)]) for j in range(3))
    first_device = f == 0
    own_scores = []
    for t in range(TILES):
        score = jnp.sum(jnp.where(own_half, query[t] * key_new[t], 0.0), axis=1, keepdims=True) * 0.125
        own_scores.append(jnp.where(first_device, score, NEG))
    smix[f], sstat[f] = attend(query, sk, sv, slots, valid, (own_scores, value_new))
    phase("mix1_x")
    frames_send(5, sstat)
    frames_send(6, smix)
    received(5, sstat, NF - 1)
    received(6, smix, NF - 1)
    phase("join1")
    self_mix = joined(smix, sstat)

    local[OW].wait()
    so_buf[f] = fold_window(nt(self_mix, pow_[...]))
    phase("so_x")
    frames_send(7, so_buf)
    received(7, so_buf, NF - 1)
    phase("ln2")
    after_self = start + jnp.concatenate(columns_joined([so_buf[k] for k in range(NF)]), axis=1)
    normed2 = norm(after_self, 1)
    local[CQW].wait()
    cq_buf[f] = fold_window(nt(normed2, pcq[...]))
    phase("cq_x")
    frames_send(8, cq_buf)
    local[CK].wait()
    local[CV].wait()
    received(8, cq_buf, NF - 1)
    phase("attn2")
    cross_query = columns_joined([cq_buf[k] for k in range(NF)])
    cmix[f], cstat[f] = attend(cross_query, ck, cv, frames, every, None)
    phase("mix2_x")
    frames_send(9, cstat)
    frames_send(10, cmix)
    received(9, cstat, NF - 1)
    received(10, cmix, NF - 1)
    phase("join2")
    cross_mix = joined(cmix, cstat)
    local[COW].wait()
    co_buf[f] = fold_window(nt(cross_mix, pco[...]))
    phase("co_x")
    frames_send(11, co_buf)
    local[UP].wait()
    local[DOWN].wait()
    received(11, co_buf, NF - 1)
    phase("mlp")
    after_cross = after_self + jnp.concatenate(columns_joined([co_buf[k] for k in range(NF)]), axis=1)

    normed3 = norm(after_cross, 2)
    raised = nn(normed3, up[...])
    active = (raised * (1.0 + lax.erf(raised * (0.5 ** 0.5))) * 0.5).astype(BF16)
    lowered = nn(active, down[...])
    half = TILES // 2

    def tile(v, t):
        return v[:, 128 * t : 128 * t + 128]

    dn_buf[f] = jnp.stack([jnp.where(low, tile(lowered, t), tile(lowered, t + half)).astype(BF16) for t in range(half)])
    phase("dn_x")
    frames_send(12, dn_buf)
    received(12, dn_buf, NF - 1)
    phase("ln4")
    summed = jnp.sum(dn_buf[...].astype(F32), axis=0)
    halves = [unfold(summed[t]) for t in range(half)]
    after_mlp = after_cross + jnp.concatenate([a for a, _ in halves] + [b for _, b in halves], axis=1)
    final = norm(after_mlp, 3).astype(F32)
    fin_buf[d] = jnp.stack([jnp.where(low, tile(final, t), tile(final, t + half)).astype(BF16) for t in range(half)])
    phase("fin_x")
    dp_send(13, fin_buf)
    received(13, fin_buf, nd - 1)

    phase("logits")
    low3 = lax.broadcasted_iota(I32, (nd // 2, 8, 128), 1) < 4
    first, second = [], []
    for t in range(half):
        both = fin_buf[:, t].astype(F32)
        turned = roll4(both).reshape(nd // 2, 2, 8, 128)
        both = both.reshape(nd // 2, 2, 8, 128)
        first.append(jnp.where(low3, both[:, 0], turned[:, 1]).reshape(nd * 4, 128))
        second.append(jnp.where(low3, turned[:, 0], both[:, 1]).reshape(nd * 4, 128))
    logits = nt(emb[...], jnp.concatenate(first + second, axis=1).astype(BF16))
    peak = jnp.max(logits, axis=0, keepdims=True)
    st1[f] = peak + jnp.log(jnp.sum(jnp.exp(logits - peak), axis=0, keepdims=True))
    phase("stats_frames")
    frames_send(14, st1)
    received(14, st1, NF - 1)

    def joined_levels(levels):
        top = jnp.max(levels, axis=0)
        return top + jnp.log(jnp.sum(jnp.exp(levels - top[None]), axis=0))

    st2[d] = joined_levels(st1[...])
    phase("stats_dp")
    dp_send(15, st2)
    received(15, st2, nd - 1)
    phase("out")
    out_ref[...] = logits - joined_levels(st2[...])

    phase("drain")
    for n, buf, count in exchanges:
        pltpu.make_async_copy(buf.at[pl.ds(0, count)], buf.at[pl.ds(0, count)], ssem.at[n]).wait()
    phase(None)


def on_device(nd, *args):
    (token_ids, positions, embed, pos_table, self_keys, self_values, cross_keys, cross_values, norm_gains, qkv_weight,
     out_weight, cross_query_weight, cross_out_weight, up_weight, down_weight) = args
    vocab = embed.shape[0]
    slots, frames, hidden = self_keys.shape[1], cross_keys.shape[1], up_weight.shape[1]
    streams = nd * 4
    vm = pltpu.VMEM
    big = (embed, pos_table, self_keys, self_values, cross_keys, cross_values, norm_gains, jnp.swapaxes(qkv_weight, 1, 2),
           out_weight.T, cross_query_weight.T, cross_out_weight.T, up_weight, down_weight)
    held = [vm(a.shape, a.dtype) for a in (embed, pos_table, self_keys, self_values, cross_keys, cross_values, norm_gains,
                                           up_weight, down_weight)]
    scratch = held + [
        vm((3, 256, WIDTH), BF16), vm((256, WIDTH), BF16), vm((256, WIDTH), BF16), vm((256, WIDTH), BF16),
        vm((nd, 8, 128), I32),
        vm((NF, vocab, 256), BF16),
        vm((nd, 8, 128), BF16), vm((nd, 8, 128), BF16),
        vm((NF, 8, 128), BF16),
        vm((NF, 3, 8, 128), BF16),
        vm((NF, TILES // 2, 8, 128), BF16), vm((NF, 8, 128), F32),
        vm((NF, 8, 128), BF16), vm((NF, 8, 128), BF16),
        vm((NF, TILES // 2, 8, 128), BF16), vm((NF, 8, 128), F32),
        vm((NF, 8, 128), BF16),
        vm((NF, TILES // 2, 8, 128), BF16),
        vm((nd, TILES // 2, 8, 128), BF16),
        vm((NF, 1, streams), F32), vm((nd, 1, streams), F32),
        pltpu.SemaphoreType.DMA((len(big),)), pltpu.SemaphoreType.DMA((16,)), pltpu.SemaphoreType.DMA((16,)),
    ]
    return pl.pallas_call(
        functools.partial(kernel, nd, vocab, slots, frames, hidden),
        out_shape=jax.ShapeDtypeStruct((vocab, streams), F32),
        in_specs=[pl.BlockSpec(memory_space=pltpu.SMEM)] * 2 + [pl.BlockSpec(memory_space=pl.ANY)] * len(big),
        out_specs=pl.BlockSpec(memory_space=pltpu.VMEM),
        scratch_shapes=scratch,
        compiler_params=pltpu.CompilerParams(collective_id=0, has_side_effects=True, vmem_limit_bytes=60 * 1024 * 1024),
    )(token_ids, positions, *big).T


def solution(mesh):
    nd = mesh.shape["dp"]
    both = ("dp", "frames")
    in_specs = (
        P("dp"), P("dp"), P(both, None), P(),
        P("dp", "frames", None), P("dp", "frames", None), P("dp", "frames", None), P("dp", "frames", None),
        P(), P(None, None, "frames"), P(None, "frames"), P(None, "frames"), P(None, "frames"), P(None, "frames"),
        P("frames", None),
    )
    return jax.shard_map(functools.partial(on_device, nd), mesh=mesh, in_specs=in_specs, out_specs=P(None, both),
                         check_vma=False)
```
